32 devices in a mesh: row: 4 (over z), col: 8 (over y, x, core).
Axes of the slice: x: 2, y: 2, z: 4, core: 2. Of those that a mesh axis runs over, the one named last changes fastest.
Arguments:
- points: float32 [131072, 64], P(('row', 'col')), may hold values from -6 to 6
- factor: float32 [131072, 512], P(('row', 'col')), may hold values from -0.06 to 0.06
- pivots: int32 [2, 128], replicated, may hold values from 0 to 131071, as said below
Outputs:
- factor_new: float32 [131072, 256], P(('row', 'col'))
- gram_rows: float32 [256, 768], replicated
The draws below stay inside these ranges and needn't reach their ends.
Inputs may be any that keep to these rules, and one draw needn't show every extreme that they name: All 256 pivots are different points.
All inputs are finite; a program needn't handle non-finite values.
Results may differ from the reference program's by a relative error of at most 0.00013.
Values sent between devices are 32-bit elements; how exact they have to be, the bound alone decides.
No kernel may reach another device: no remote copies, remote signals or barrier semaphores. Data moves between devices by JAX's collectives and lax.ppermute only.
A program may use at most 128 MiB of HBM per device.

```python
import jax
import jax.numpy as jnp
from jax import lax

DIM = 64
RANK = 512
BLOCK = 128
BLOCKS = 2
PTS_DEV = 4096
NPTS = 131072


def draw_pivots(key, part):
    chosen = jax.random.choice(key, NPTS, (BLOCKS * BLOCK,), replace=False)
    return chosen.reshape(BLOCKS, BLOCK).astype(jnp.int32)


def shard_levels(key, shape, shards, smallest, largest):
    gain = 1.0
    for position, shards_of in shards:
        heights = jax.random.uniform(jax.random.fold_in(jax.random.fold_in(key, 6), position), (shards_of,), jnp.float32, smallest / len(shards), largest / len(shards))
        gain = gain * jnp.repeat(jnp.exp(heights), shape[position] // shards_of).reshape((-1,) + (1,) * (len(shape) - 1 - position))
    return gain


def normal_values(rng, dims, deviation, bound, split=(), held_as=jnp.bfloat16):
    drawn = deviation * jax.random.normal(rng, dims, jnp.float32)
    if split:
        drawn = drawn * shard_levels(rng, dims, split, -0.22, 0.18)
    return jnp.clip(drawn, -bound, bound).astype(held_as)


def setup_inputs(seed: int = 0) -> dict:
    keys = jax.random.split(jax.random.key(seed), 4)
    return {
        "points": normal_values(keys[0], (NPTS, DIM), 1.0, 6.0, ((0, 32),), jnp.float32),
        "factor": normal_values(keys[1], (NPTS, RANK), 0.01, 0.06, ((0, 32),), jnp.float32),
        "pivots": draw_pivots(jax.random.fold_in(keys[3], 71), 0),
    }


highest = lax.Precision.HIGHEST
nugget = 0.1

def kernel_block(left, right):
    cross = jnp.dot(left, right.T, precision=highest)
    dist = jnp.sum(left * left, 1)[:, None] + jnp.sum(right * right, 1)[None, :] - 2.0 * cross
    return jnp.exp(-dist / left.shape[1])

def pivot_inverse(pivot_points, pivot_factor):
    size = pivot_points.shape[0]
    identity = jnp.eye(size, dtype=jnp.float32)
    outer = jnp.dot(pivot_factor, pivot_factor.T, precision=highest)
    shift = nugget + jnp.max(jnp.sum(jnp.abs(outer), 1))
    core = kernel_block(pivot_points, pivot_points) - outer + shift * identity
    lower = jnp.linalg.cholesky(core)
    return jax.scipy.linalg.solve_triangular(lower, identity, lower=True)

def new_columns(rows_points, rows_factor, pivot_points, pivot_factor, inverse):
    resid = kernel_block(rows_points, pivot_points) - jnp.dot(rows_factor, pivot_factor.T, precision=highest)
    return jnp.dot(resid, inverse.T, precision=highest)

def reference(points, factor, pivots):
    current = factor
    made = []
    for section in range(BLOCKS):
        indices = pivots[section].astype(jnp.int32)
        pivot_points = points[indices]
        pivot_factor = current[indices]
        inverse = pivot_inverse(pivot_points, pivot_factor)
        fresh = new_columns(points, current, pivot_points, pivot_factor, inverse)
        made.append(fresh)
        current = jnp.concatenate([current, fresh], 1)
    factor_new = jnp.concatenate(made, 1)
    gram_rows = jnp.dot(factor_new.T, current, precision=highest) / PTS_DEV
    return (factor_new, gram_rows)
```

```python
import functools

import jax
import jax.numpy as jnp
from jax import lax
from jax.experimental import pallas as pl
from jax.experimental.pallas import tpu as pltpu
from jax.sharding import PartitionSpec as P

AXES = ("row", "col")
nugget = 0.1
highest = lax.Precision.HIGHEST
panel_rows = 16
halvings = 3


def split2(x):
    a = x.astype(jnp.bfloat16)
    return a, (x - a.astype(jnp.float32)).astype(jnp.bfloat16)


def split3(x):
    a = x.astype(jnp.bfloat16)
    rest = x - a.astype(jnp.float32)
    b = rest.astype(jnp.bfloat16)
    return a, b, (rest - b.astype(jnp.float32)).astype(jnp.bfloat16)


def contract(x, y, dim_x, dim_y, precision=None):
    return lax.dot_general(
        x, y, (((dim_x,), (dim_y,)), ((), ())), precision=precision, preferred_element_type=jnp.float32
    )


def pick_kernel(first_ref, pivots_ref, points_ref, factor_ref, local_ref, out_ref, sem):
    width, count = points_ref.shape
    rank = factor_ref.shape[1]
    total = out_ref.shape[0]
    first = first_ref[0]
    out_ref[...] = jnp.zeros_like(out_ref)

    def copy(k):
        local = pivots_ref[k] - first
        inside = (local >= 0) & (local < count)
        row = jnp.clip(local, 0, count - 1)
        dma = pltpu.make_async_copy(factor_ref.at[pl.ds(row, 1), :], out_ref.at[pl.ds(k, 1), pl.ds(0, rank)], sem)
        return inside, dma

    def start(k, _):
        inside, dma = copy(k)

        @pl.when(inside)
        def _():
            dma.start()

        return 0

    def wait(k, _):
        inside, dma = copy(k)

        @pl.when(inside)
        def _():
            dma.wait()

        return 0

    lax.fori_loop(0, total, start, 0)
    chunk = 512
    picked = jnp.zeros((total, width), jnp.float32)
    for base in range(0, count, chunk):
        which = lax.broadcasted_iota(jnp.int32, (total, chunk), 1) + base
        hot = jnp.where(which == local_ref[...], 1.0, 0.0).astype(jnp.bfloat16)
        for part in split3(points_ref[:, base : base + chunk]):
            picked = picked + contract(hot, part, 1, 1)
    lax.fori_loop(0, total, wait, 0)
    out_ref[:, rank : rank + width] = picked


def pick_rows(points_t, factor, pivots, first):
    width, count = points_t.shape
    rank = factor.shape[1]
    total = pivots.shape[0]
    lanes = rank + -(-width // 128) * 128
    local = (pivots - first)[:, None]
    return pl.pallas_call(
        pick_kernel,
        in_specs=[
            pl.BlockSpec(memory_space=pltpu.SMEM),
            pl.BlockSpec(memory_space=pltpu.SMEM),
            pl.BlockSpec(memory_space=pltpu.VMEM),
            pl.BlockSpec(memory_space=pl.ANY),
            pl.BlockSpec(memory_space=pltpu.VMEM),
        ],
        out_specs=pl.BlockSpec(memory_space=pltpu.VMEM),
        out_shape=jax.ShapeDtypeStruct((total, lanes), jnp.float32),
        scratch_shapes=[pltpu.SemaphoreType.DMA],
        name="pick_rows",
    )(first[None], pivots, points_t, factor, local)


def residual_kernel(points_ref, factor_ref, pivot_ref, res_ref, sum_ref, wide, last, high, low, norm):
    width = points_ref.shape[0]
    rank = factor_ref.shape[1]

    @pl.when(pl.program_id(0) == 0)
    def _():
        p = pivot_ref[:, rank : rank + width]
        norm[...] = contract(jnp.ones((8, width), jnp.float32), p * p, 1, 1, highest)
        a, b, c = split3(-2.0 * p)
        one = jnp.ones(a.shape, jnp.bfloat16)
        wide[...] = jnp.concatenate([a, a, b, b], 1)
        last[...] = jnp.concatenate([c, a, one, one], 1)
        high[...], low[...] = split2(pivot_ref[:, :rank])
        sum_ref[...] = jnp.zeros_like(sum_ref)

    x = points_ref[...]
    a, b, c = split3(x)
    sq = jnp.sum(x * x, 0, keepdims=True)
    n1, n2, n3 = split3(sq)
    row = lax.broadcasted_iota(jnp.int32, (2 * width, x.shape[1]), 0)
    zero = jnp.zeros((), jnp.bfloat16)
    norms = jnp.where(row == 0, n1, jnp.where(row == 1, n2, jnp.where(row == 2, n3, zero)))
    dist = contract(jnp.concatenate([a, b, a, b], 0), wide[...], 0, 1)
    dist = dist + contract(jnp.concatenate([a, c, norms], 0), last[...], 0, 1)
    dist = dist + norm[0:1, :]
    kern = jnp.exp(-dist / width)
    fh, fl = split2(factor_ref[...])
    qh = high[...]
    res = kern - (contract(fh, qh, 1, 1) + (contract(fh, low[...], 1, 1) + contract(fl, qh, 1, 1)))
    res_ref[...] = res
    rh, rl = split2(res)
    sum_ref[:, :rank] += contract(rh, fh, 0, 0) + (contract(rh, fl, 0, 0) + contract(rl, fh, 0, 0))
    sum_ref[:, rank:] += contract(rh, rh, 0, 0) + (contract(rh, rl, 0, 0) + contract(rl, rh, 0, 0))


def residuals(points_t, factor, fetched):
    width, count = points_t.shape
    rank = factor.shape[1]
    total, lanes = fetched.shape
    tile = min(1024, count)
    bf16 = jnp.bfloat16
    return pl.pallas_call(
        residual_kernel,
        grid=(count // tile,),
        in_specs=[
            pl.BlockSpec((width, tile), lambda i: (0, i)),
            pl.BlockSpec((tile, rank), lambda i: (i, 0)),
            pl.BlockSpec((total, lanes), lambda i: (0, 0)),
        ],
        out_specs=[
            pl.BlockSpec((tile, total), lambda i: (i, 0)),
            pl.BlockSpec((total, rank + total), lambda i: (0, 0)),
        ],
        out_shape=[
            jax.ShapeDtypeStruct((count, total), jnp.float32),
            jax.ShapeDtypeStruct((total, rank + total), jnp.float32),
        ],
        scratch_shapes=[
            pltpu.VMEM((total, 4 * width), bf16),
            pltpu.VMEM((total, 4 * width), bf16),
            pltpu.VMEM((total, rank), bf16),
            pltpu.VMEM((total, rank), bf16),
            pltpu.VMEM((8, total), jnp.float32),
        ],
        name="residuals",
    )(points_t, factor, fetched)


def invert_factor(work, size):
    step = panel_rows
    for start in range(0, size, step):
        after = start + step
        panel = work[start:after, :]
        rows = lax.broadcasted_iota(jnp.int32, (step, size), 0)
        cols = [jnp.broadcast_to(panel[:, start + k : start + k + 1], (step, size)) for k in range(step)]
        left = panel[:, :size]
        right = panel[:, size:]
        scale = jnp.zeros((step, size), jnp.float32)
        solved = jnp.zeros((step, size), jnp.float32)
        for j in range(step):
            here = rows == j
            root = lax.rsqrt(jnp.broadcast_to(cols[j][j : j + 1], (step, size)))
            inv = root * root
            mult = jnp.where(here, 0.0, cols[j] * inv)
            scale = jnp.where(here, inv, scale)
            pivot_right = jnp.broadcast_to(right[j : j + 1], (step, size))
            solved = jnp.where(here, pivot_right * root, solved)
            for k in range(j + 1, step):
                cols[k] = cols[k] - mult * jnp.broadcast_to(cols[k][j : j + 1], (step, size))
            left = left - mult * jnp.broadcast_to(left[j : j + 1], (step, size))
            right = right - mult * pivot_right
        work[start:after, size:] = solved
        if after < size:
            parts = split3(jnp.concatenate([left * scale, right * scale], 1))
            above = [jnp.zeros((start, 2 * size), jnp.bfloat16)] if start else []
            below = [jnp.zeros((size - after, 2 * size), jnp.bfloat16)]
            e1, e2, e3 = [jnp.concatenate(above + [part] + below, 0) for part in parts]
            a1, a2, a3 = split3(work[after:, :size])
            update = contract(a1, e1, 1, 0) + (contract(a1, e2, 1, 0) + contract(a2, e1, 1, 0))
            update = update + (contract(a1, e3, 1, 0) + contract(a2, e2, 1, 0) + contract(a3, e1, 1, 0))
            work[after:, :] = work[after:, :] - update


def inverse_kernel(width, size, pivot_ref, inv_ref, work):
    total = pivot_ref.shape[0]
    rank = pivot_ref.shape[1] - -(-width // 128) * 128
    p = pivot_ref[:, rank : rank + width]
    q = pivot_ref[:, :rank]
    sq = p * p
    norm_row = contract(jnp.ones((8, width), jnp.float32), sq, 1, 1, highest)[0:1]
    norm_col = jnp.sum(sq, 1, keepdims=True)
    kern = jnp.exp(-(norm_col + norm_row - 2.0 * contract(p, p, 1, 1, highest)) / width)
    outer = contract(q, q, 1, 1, highest)
    eye = jnp.where(
        lax.broadcasted_iota(jnp.int32, (size, size), 0) == lax.broadcasted_iota(jnp.int32, (size, size), 1), 1.0, 0.0
    )
    inv_ref[...] = jnp.zeros_like(inv_ref)
    for begin in range(0, total, size):
        end = begin + size
        block = outer[begin:end, begin:end]
        if begin:
            before = inv_ref[:begin, :begin]
            mixed = contract(kern[begin:end, :begin] - outer[begin:end, :begin], before, 1, 1, highest)
            block = block + contract(mixed, mixed, 1, 1, highest)
        shift = nugget + jnp.max(jnp.sum(jnp.abs(block), 1, keepdims=True), axis=0, keepdims=True)
        work[:, :size] = kern[begin:end, begin:end] - block + shift * eye
        work[:, size:] = eye
        invert_factor(work, size)
        inverse = work[:, size:]
        inv_ref[begin:end, begin:end] = inverse
        if begin:
            inv_ref[begin:end, :begin] = -contract(inverse, contract(mixed, before, 1, 0, highest), 1, 0, highest)


def joint_inverse(fetched, width, size):
    total = fetched.shape[0]
    return pl.pallas_call(
        functools.partial(inverse_kernel, width, size),
        out_shape=jax.ShapeDtypeStruct((total, total), jnp.float32),
        scratch_shapes=[pltpu.VMEM((size, 2 * size), jnp.float32)],
        name="joint_inverse",
    )(fetched)


def columns_kernel(res_ref, inv_ref, out_ref, one, two, three):
    @pl.when(pl.program_id(0) == 0)
    def _():
        one[...], two[...], three[...] = split3(inv_ref[...])

    a, b, c = split3(res_ref[...])
    out = contract(a, one[...], 1, 1) + (contract(a, two[...], 1, 1) + contract(b, one[...], 1, 1))
    out_ref[...] = out + (contract(b, two[...], 1, 1) + contract(a, three[...], 1, 1) + contract(c, one[...], 1, 1))


def new_columns(res, inv):
    count, total = res.shape
    tile = min(1024, count)
    return pl.pallas_call(
        columns_kernel,
        grid=(count // tile,),
        in_specs=[pl.BlockSpec((tile, total), lambda i: (i, 0)), pl.BlockSpec((total, total), lambda i: (0, 0))],
        out_specs=pl.BlockSpec((tile, total), lambda i: (i, 0)),
        out_shape=jax.ShapeDtypeStruct((count, total), jnp.float32),
        scratch_shapes=[pltpu.VMEM((total, total), jnp.bfloat16)] * 3,
        name="new_columns",
    )(res, inv)


def gram_kernel(count, sum_ref, inv_ref, out_ref):
    inv = inv_ref[...]
    rank = sum_ref.shape[1] - inv.shape[0]
    half = contract(inv, sum_ref[...], 1, 0, highest)
    out_ref[:, :rank] = half[:, :rank] / count
    out_ref[:, rank:] = contract(half[:, rank:], inv, 1, 1, highest) / count


def gram_rows(sums, inv, count):
    return pl.pallas_call(
        functools.partial(gram_kernel, count),
        out_shape=jax.ShapeDtypeStruct(sums.shape, jnp.float32),
        name="gram_rows",
    )(sums, inv)


def sum_over_devices(x, index, bits):
    swap = lambda piece, bit: lax.ppermute(piece, AXES, [(i, i ^ (1 << bit)) for i in range(1 << bits)])
    near = min(halvings, bits)
    for bit in range(near):
        half = x.shape[0] // 2
        mine = (index >> bit) & 1
        sent = lax.dynamic_slice_in_dim(x, (1 - mine) * half, half, 0)
        x = lax.dynamic_slice_in_dim(x, mine * half, half, 0) + swap(sent, bit)
    for bit in range(near, bits):
        x = x + swap(x, bit)
    for bit in reversed(range(near)):
        mine = (index >> bit) & 1
        other = swap(x, bit)
        x = jnp.concatenate([jnp.where(mine == 0, x, other), jnp.where(mine == 0, other, x)], 0)
    return x


def body(bits, points, factor, pivots):
    count, width = points.shape
    size = pivots.shape[1]
    index = lax.axis_index("row") * lax.axis_size("col") + lax.axis_index("col")
    points_t = points.T
    picked = pick_rows(points_t, factor, pivots.reshape(-1), (index * count).astype(jnp.int32))
    fetched = sum_over_devices(picked, index, bits)
    res, sums = residuals(points_t, factor, fetched)
    inv = joint_inverse(fetched, width, size)
    total = sum_over_devices(sums, index, bits)
    return new_columns(res, inv), gram_rows(total, inv, count)


def solution(mesh):
    bits = (mesh.size - 1).bit_length()
    assert mesh.size == 1 << bits
    in_specs = (P(AXES, None), P(AXES, None), P())
    out_specs = (P(AXES, None), P())
    return jax.shard_map(
        functools.partial(body, bits), mesh=mesh, in_specs=in_specs, out_specs=out_specs, check_vma=False
    )
```

```python
import functools

import jax
import jax.numpy as jnp
from jax import lax
from jax.experimental import pallas as pl
from jax.experimental.pallas import tpu as pltpu
from jax.sharding import PartitionSpec as P

AXES = ("row", "col")
nugget = 0.1
highest = lax.Precision.HIGHEST
panel_rows = 16
halvings = 3


def split2(x):
    a = x.astype(jnp.bfloat16)
    return a, (x - a.astype(jnp.float32)).astype(jnp.bfloat16)


def split3(x):
    a = x.astype(jnp.bfloat16)
    rest = x - a.astype(jnp.float32)
    b = rest.astype(jnp.bfloat16)
    return a, b, (rest - b.astype(jnp.float32)).astype(jnp.bfloat16)


def contract(x, y, dim_x, dim_y, precision=None):
    return lax.dot_general(
        x, y, (((dim_x,), (dim_y,)), ((), ())), precision=precision, preferred_element_type=jnp.float32
    )


def pick_kernel(pivots_ref, pivots_row_ref, points_ref, factor_ref, keep_ref, send_ref, rows_ref, sem):
    width, count = points_ref.shape
    rank = factor_ref.shape[1]
    total = rows_ref.shape[0]
    half = total // 2
    index = lax.axis_index("row") * lax.axis_size("col") + lax.axis_index("col")
    first = index * count
    rows_ref[:, :rank] = jnp.zeros((total, rank), jnp.float32)

    def copy(row, k):
        return pltpu.make_async_copy(factor_ref.at[pl.ds(row, 1), :], rows_ref.at[pl.ds(k, 1), pl.ds(0, rank)], sem)

    def start(k, started):
        local = pivots_ref[k] - first
        inside = (local >= 0) & (local < count)

        @pl.when(inside)
        def _():
            copy(local, k).start()

        return started + inside.astype(jnp.int32)

    started = lax.fori_loop(0, total, start, 0, unroll=8)
    chunk = min(512, count)
    picked = jnp.zeros((3 * width, total), jnp.float32)
    local_row = pivots_row_ref[...] - first
    for base in range(0, count, chunk):
        which = lax.broadcasted_iota(jnp.int32, (chunk, total), 0) + base
        hot = jnp.where(which == local_row, 1.0, 0.0).astype(jnp.bfloat16)
        picked = picked + contract(jnp.concatenate(split3(points_ref[:, base : base + chunk]), 0), hot, 1, 0)
    point = picked[:width] + picked[width : 2 * width] + picked[2 * width :]
    spare = rows_ref.shape[1] - rank - width
    rows_ref[:, rank:] = jnp.concatenate([point, jnp.zeros((spare, total), jnp.float32)], 0).T

    def wait(k, _):
        copy(0, 0).wait()
        return 0

    lax.fori_loop(0, started, wait, 0)
    mine = index & 1
    keep_ref[...] = rows_ref[pl.ds(pl.multiple_of(mine * half, 8), half), :]
    send_ref[...] = rows_ref[pl.ds(pl.multiple_of((1 - mine) * half, 8), half), :]


def pick_rows(points_t, factor, pivots):
    rank = factor.shape[1]
    total = pivots.shape[0]
    lanes = rank + -(-points_t.shape[0] // 128) * 128
    vmem = pl.BlockSpec(memory_space=pltpu.VMEM)
    return pl.pallas_call(
        pick_kernel,
        in_specs=[pl.BlockSpec(memory_space=pltpu.SMEM), vmem, vmem, pl.BlockSpec(memory_space=pl.ANY)],
        out_specs=[vmem, vmem],
        out_shape=[jax.ShapeDtypeStruct((total // 2, lanes), jnp.float32)] * 2,
        scratch_shapes=[pltpu.VMEM((total, lanes), jnp.float32), pltpu.SemaphoreType.DMA],
        name="pick_rows",
    )(pivots, pivots[None], points_t, factor)


def residual_kernel(
    points_ref, factor_ref, pivot_ref, res_ref, keep_ref, send_ref, sum_ref, wide, last, high, low, norm
):
    width = points_ref.shape[0]
    rank = factor_ref.shape[1]

    @pl.when(pl.program_id(0) == 0)
    def _():
        p = pivot_ref[:, rank : rank + width]
        norm[...] = contract(jnp.ones((8, width), jnp.float32), p * p, 1, 1, highest)
        a, b, c = split3(-2.0 * p)
        one = jnp.ones(a.shape, jnp.bfloat16)
        wide[...] = jnp.concatenate([a, a, b, b], 1)
        last[...] = jnp.concatenate([c, a, one, one], 1)
        high[...], low[...] = split2(pivot_ref[:, :rank])
        sum_ref[...] = jnp.zeros_like(sum_ref)

    x = points_ref[...]
    a, b, c = split3(x)
    sq = jnp.sum(x * x, 0, keepdims=True)
    n1, n2, n3 = split3(sq)
    row = lax.broadcasted_iota(jnp.int32, (2 * width, x.shape[1]), 0)
    zero = jnp.zeros((), jnp.bfloat16)
    norms = jnp.where(row == 0, n1, jnp.where(row == 1, n2, jnp.where(row == 2, n3, zero)))
    dist = contract(jnp.concatenate([a, b, a, b], 0), wide[...], 0, 1)
    dist = dist + contract(jnp.concatenate([a, c, norms], 0), last[...], 0, 1)
    dist = dist + norm[0:1, :]
    kern = jnp.exp(-dist / width)
    fh, fl = split2(factor_ref[...])
    qh = high[...]
    res = kern - (contract(fh, qh, 1, 1) + (contract(fh, low[...], 1, 1) + contract(fl, qh, 1, 1)))
    res_ref[...] = res
    rh, rl = split2(res)
    sum_ref[:, :rank] += contract(rh, fh, 0, 0) + (contract(rh, fl, 0, 0) + contract(rl, fh, 0, 0))
    sum_ref[:, rank:] += contract(rh, rh, 0, 0) + (contract(rh, rl, 0, 0) + contract(rl, rh, 0, 0))

    @pl.when(pl.program_id(0) == pl.num_programs(0) - 1)
    def _():
        half = sum_ref.shape[0] // 2
        mine = (lax.axis_index("row") * lax.axis_size("col") + lax.axis_index("col")) & 1
        keep_ref[...] = sum_ref[pl.ds(pl.multiple_of(mine * half, 8), half), :]
        send_ref[...] = sum_ref[pl.ds(pl.multiple_of((1 - mine) * half, 8), half), :]


def residuals(points_t, factor, fetched):
    width, count = points_t.shape
    rank = factor.shape[1]
    total, lanes = fetched.shape
    tile = min(1024, count)
    bf16 = jnp.bfloat16
    return pl.pallas_call(
        residual_kernel,
        grid=(count // tile,),
        in_specs=[
            pl.BlockSpec((width, tile), lambda i: (0, i)),
            pl.BlockSpec((tile, rank), lambda i: (i, 0)),
            pl.BlockSpec((total, lanes), lambda i: (0, 0)),
        ],
        out_specs=[
            pl.BlockSpec((tile, total), lambda i: (i, 0)),
            pl.BlockSpec((total // 2, rank + total), lambda i: (0, 0)),
            pl.BlockSpec((total // 2, rank + total), lambda i: (0, 0)),
        ],
        out_shape=[
            jax.ShapeDtypeStruct((count, total), jnp.float32),
            jax.ShapeDtypeStruct((total // 2, rank + total), jnp.float32),
            jax.ShapeDtypeStruct((total // 2, rank + total), jnp.float32),
        ],
        scratch_shapes=[
            pltpu.VMEM((total, rank + total), jnp.float32),
            pltpu.VMEM((total, 4 * width), bf16),
            pltpu.VMEM((total, 4 * width), bf16),
            pltpu.VMEM((total, rank), bf16),
            pltpu.VMEM((total, rank), bf16),
            pltpu.VMEM((8, total), jnp.float32),
        ],
        name="residuals",
    )(points_t, factor, fetched)


def eliminate(work, size, begin, end):
    step = panel_rows
    for start in range(begin, end, step):
        after = start + step
        panel = work[start:after, :]
        rows = lax.broadcasted_iota(jnp.int32, (step, size), 0)
        cols = [jnp.broadcast_to(panel[:, start + k : start + k + 1], (step, size)) for k in range(step)]
        left = panel[:, :size]
        right = panel[:, size:]
        scale = jnp.zeros((step, size), jnp.float32)
        solved = jnp.zeros((step, size), jnp.float32)
        for j in range(step):
            here = rows == j
            root = lax.rsqrt(jnp.broadcast_to(cols[j][j : j + 1], (step, size)))
            inv = root * root
            mult = jnp.where(here, 0.0, cols[j] * inv)
            scale = jnp.where(here, inv, scale)
            pivot_right = jnp.broadcast_to(right[j : j + 1], (step, size))
            solved = jnp.where(here, pivot_right * root, solved)
            for k in range(j + 1, step):
                cols[k] = cols[k] - mult * jnp.broadcast_to(cols[k][j : j + 1], (step, size))
            left = left - mult * jnp.broadcast_to(left[j : j + 1], (step, size))
            right = right - mult * pivot_right
        work[start:after, size:] = solved
        if after < size:
            parts = split3(jnp.concatenate([left * scale, right * scale], 1))
            above = [jnp.zeros((start, 2 * size), jnp.bfloat16)] if start else []
            below = [jnp.zeros((size - after, 2 * size), jnp.bfloat16)]
            e1, e2, e3 = [jnp.concatenate(above + [part] + below, 0) for part in parts]
            a1, a2, a3 = split3(work[after:, :size])
            update = contract(a1, e1, 1, 0) + (contract(a1, e2, 1, 0) + contract(a2, e1, 1, 0))
            update = update + (contract(a1, e3, 1, 0) + contract(a2, e2, 1, 0) + contract(a3, e1, 1, 0))
            work[after:, :] = work[after:, :] - update


def pairs_kernel(width, pivot_ref, kern_ref, outer_ref):
    rank = pivot_ref.shape[1] - -(-width // 128) * 128
    p = pivot_ref[:, rank : rank + width]
    q = pivot_ref[:, :rank]
    sq = p * p
    norm_row = contract(jnp.ones((8, width), jnp.float32), sq, 1, 1, highest)[0:1]
    norm_col = jnp.sum(sq, 1, keepdims=True)
    kern_ref[...] = jnp.exp(-(norm_col + norm_row - 2.0 * contract(p, p, 1, 1, highest)) / width)
    outer_ref[...] = contract(q, q, 1, 1, highest)


def pivot_pairs(fetched, width):
    total = fetched.shape[0]
    return pl.pallas_call(
        functools.partial(pairs_kernel, width),
        out_shape=[jax.ShapeDtypeStruct((total, total), jnp.float32)] * 2,
        name="pivot_pairs",
    )(fetched)


def block_kernel(begin, size, rows, *refs):
    kern_ref, outer_ref = refs[:2]
    end = begin + size
    block = outer_ref[begin:end, begin:end]
    if begin:
        before_ref, work_ref, mixed_ref = refs[2:]
        mixed = contract(
            kern_ref[begin:end, :begin] - outer_ref[begin:end, :begin], before_ref[...], 1, 1, highest
        )
        mixed_ref[...] = mixed
        block = block + contract(mixed, mixed, 1, 1, highest)
    else:
        work_ref = refs[2]
    eye = jnp.where(
        lax.broadcasted_iota(jnp.int32, (size, size), 0) == lax.broadcasted_iota(jnp.int32, (size, size), 1), 1.0, 0.0
    )
    shift = nugget + jnp.max(jnp.sum(jnp.abs(block), 1, keepdims=True), axis=0, keepdims=True)
    work_ref[:, :size] = kern_ref[begin:end, begin:end] - block + shift * eye
    work_ref[:, size:] = eye
    eliminate(work_ref, size, 0, rows)


def open_block(kern, outer, before, begin, size, rows):
    shapes = [jax.ShapeDtypeStruct((size, 2 * size), jnp.float32)]
    args = (kern, outer)
    if begin:
        shapes.append(jax.ShapeDtypeStruct((size, begin), jnp.float32))
        args = (kern, outer, before)
    return pl.pallas_call(functools.partial(block_kernel, begin, size, rows), out_shape=shapes, name="open_block")(*args)


def close_kernel(begin, size, rows, done_ref, mixed_ref, before_ref, inv_ref, work):
    work[...] = done_ref[...]
    eliminate(work, size, rows, size)
    inverse = work[:, size:]
    before = before_ref[...]
    inv_ref[:begin, :begin] = before
    inv_ref[:begin, begin:] = jnp.zeros((begin, size), jnp.float32)
    inv_ref[begin:, begin:] = inverse
    inv_ref[begin:, :begin] = -contract(inverse, contract(mixed_ref[...], before, 1, 0, highest), 1, 0, highest)


def close_block(done, mixed, before, begin, size, rows):
    end = begin + size
    return pl.pallas_call(
        functools.partial(close_kernel, begin, size, rows),
        out_shape=jax.ShapeDtypeStruct((end, end), jnp.float32),
        scratch_shapes=[pltpu.VMEM((size, 2 * size), jnp.float32)],
        name="close_block",
    )(done, mixed, before)


def columns_kernel(res_ref, inv_ref, *refs):
    out_ref, one, two, three = refs[-4:]

    @pl.when(pl.program_id(0) == 0)
    def _():
        one[...], two[...], three[...] = split3(inv_ref[...])

    a, b, c = split3(res_ref[...])
    out = contract(a, one[...], 1, 1) + (contract(a, two[...], 1, 1) + contract(b, one[...], 1, 1))
    out_ref[...] = out + (contract(b, two[...], 1, 1) + contract(a, three[...], 1, 1) + contract(c, one[...], 1, 1))


def new_columns(res, inv, made, tile, begin, end):
    count, total = res.shape
    in_specs = [
        pl.BlockSpec((tile, total), lambda i: (i + begin, 0)),
        pl.BlockSpec((total, total), lambda i: (0, 0)),
    ]
    args = (res, inv)
    if made is not None:
        in_specs.append(pl.BlockSpec(memory_space=pl.ANY))
        args = (res, inv, made)
    return pl.pallas_call(
        columns_kernel,
        grid=(end - begin,),
        in_specs=in_specs,
        out_specs=pl.BlockSpec((tile, total), lambda i: (i + begin, 0)),
        out_shape=jax.ShapeDtypeStruct((count, total), jnp.float32),
        scratch_shapes=[pltpu.VMEM((total, total), jnp.bfloat16)] * 3,
        input_output_aliases={} if made is None else {2: 0},
        name="new_columns",
    )(*args)


def gram_kernel(count, sum_ref, inv_ref, out_ref):
    inv = inv_ref[...]
    rank = sum_ref.shape[1] - inv.shape[0]
    half = contract(inv, sum_ref[...], 1, 0, highest)
    out_ref[:, :rank] = half[:, :rank] / count
    out_ref[:, rank:] = contract(half[:, rank:], inv, 1, 1, highest) / count


def gram_rows(sums, inv, count):
    return pl.pallas_call(
        functools.partial(gram_kernel, count),
        out_shape=jax.ShapeDtypeStruct(sums.shape, jnp.float32),
        name="gram_rows",
    )(sums, inv)


def sum_over_devices(keep, send, index, bits, work=None):
    def swap(piece, mask):
        pairs = [(i, i ^ mask) for i in range(1 << bits)]
        if work is None or not work.steps:
            return lax.ppermute(piece, AXES, pairs)
        piece, work.state = lax.optimization_barrier((piece, work.state))
        got = lax.ppermute(piece, AXES, pairs)
        work.run()
        got, work.state = lax.optimization_barrier((got, work.state))
        return got

    near = min(halvings, bits)
    x = keep + swap(send, 1)
    for bit in range(1, near):
        half = x.shape[0] // 2
        mine = (index >> bit) & 1
        sent = lax.dynamic_slice_in_dim(x, (1 - mine) * half, half, 0)
        x = lax.dynamic_slice_in_dim(x, mine * half, half, 0) + swap(sent, 1 << bit)
    for bit in range(near, bits):
        x = x + swap(x, 1 << bit)
    for bit in reversed(range(near)):
        mine = (index >> bit) & 1
        other = swap(x, 1 << bit)
        x = jnp.concatenate([jnp.where(mine == 0, x, other), jnp.where(mine == 0, other, x)], 0)
    return x


class Work:
    def __init__(self, state, steps):
        self.state = state
        self.steps = list(steps)

    def run(self):
        self.state = self.steps.pop(0)(self.state)


def body(bits, points, factor, pivots):
    count, width = points.shape
    blocks, size = pivots.shape
    index = lax.axis_index("row") * lax.axis_size("col") + lax.axis_index("col")
    points_t = points.T
    fetched = sum_over_devices(*pick_rows(points_t, factor, pivots.reshape(-1)), index, bits)
    res, keep, send = residuals(points_t, factor, fetched)

    def pairs(state):
        return dict(state, pairs=pivot_pairs(state.pop("fetched"), width))

    def first_block(state):
        (done,) = open_block(*state["pairs"], None, 0, size, size)
        return dict(state, inv=done[:, size:])

    def open_next(begin):
        def run(state):
            return dict(state, open=open_block(*state["pairs"], state["inv"], begin, size, size // 2))

        return run

    def close_next(begin):
        def run(state):
            done, mixed = state.pop("open")
            return dict(state, inv=close_block(done, mixed, state["inv"], begin, size, size // 2))

        return run

    tile = min(1024, count)
    tiles = count // tile
    cuts = [0, tiles // 4, tiles // 2, tiles]

    def columns(begin, end):
        def run(state):
            return dict(state, made=new_columns(state["res"], state["inv"], state["made"], tile, begin, end))

        return run

    steps = [pairs, first_block]
    for begin in range(size, blocks * size, size):
        steps += [open_next(begin), close_next(begin)]
    steps += [columns(b, e) for b, e in zip(cuts, cuts[1:]) if e > b]
    work = Work({"fetched": fetched, "res": res, "made": None}, steps)
    total = sum_over_devices(keep, send, index, bits, work)
    while work.steps:
        work.run()
    return work.state["made"], gram_rows(total, work.state["inv"], count)


def solution(mesh):
    bits = (mesh.size - 1).bit_length()
    assert mesh.size == 1 << bits
    in_specs = (P(AXES, None), P(AXES, None), P())
    out_specs = (P(AXES, None), P())
    return jax.shard_map(
        functools.partial(body, bits), mesh=mesh, in_specs=in_specs, out_specs=out_specs, check_vma=False
    )
```

```python
import functools

import jax
import jax.numpy as jnp
from jax import lax
from jax.experimental import pallas as pl
from jax.experimental.pallas import tpu as pltpu
from jax.sharding import PartitionSpec as P

AXES = ("row", "col")
nugget = 0.1
highest = lax.Precision.HIGHEST
panel_rows = 16
halvings = 3
vmem_bytes = 32 << 20


def split2(x):
    a = x.astype(jnp.bfloat16)
    return a, (x - a.astype(jnp.float32)).astype(jnp.bfloat16)


def split3(x):
    a = x.astype(jnp.bfloat16)
    rest = x - a.astype(jnp.float32)
    b = rest.astype(jnp.bfloat16)
    return a, b, (rest - b.astype(jnp.float32)).astype(jnp.bfloat16)


def near_by(*shape):
    return pltpu.VMEM(shape, jnp.float32)


def position():
    return lax.axis_index("row") * lax.axis_size("col") + lax.axis_index("col")


def join(out_ref, mine_ref, other_ref):
    half = mine_ref.shape[0]
    mine = position() & 1
    out_ref[pl.ds(pl.multiple_of(mine * half, 8), half), :] = mine_ref[...]
    out_ref[pl.ds(pl.multiple_of((1 - mine) * half, 8), half), :] = other_ref[...]


def contract(x, y, dim_x, dim_y, precision=None):
    return lax.dot_general(
        x, y, (((dim_x,), (dim_y,)), ((), ())), precision=precision, preferred_element_type=jnp.float32
    )


def pick_kernel(
    pivots_ref, pivots_row_ref, points_ref, factor_ref, keep_ref, send_ref, rows_ref, local_ref, sem, points_sem
):
    width, count = points_ref.shape
    rank = factor_ref.shape[1]
    total = rows_ref.shape[0]
    half = total // 2
    index = position()
    first = index * count
    points_copy = pltpu.make_async_copy(points_ref, local_ref, points_sem)
    points_copy.start()
    rows_ref[:, :rank] = jnp.zeros((total, rank), jnp.float32)

    def copy(row, k):
        return pltpu.make_async_copy(factor_ref.at[pl.ds(row, 1), :], rows_ref.at[pl.ds(k, 1), pl.ds(0, rank)], sem)

    def start(k, started):
        local = pivots_ref[k] - first
        inside = (local >= 0) & (local < count)

        @pl.when(inside)
        def _():
            copy(local, k).start()

        return started + inside.astype(jnp.int32)

    started = lax.fori_loop(0, total, start, 0, unroll=8)
    chunk = min(512, count)
    picked = jnp.zeros((3 * width, total), jnp.float32)
    local_row = pivots_row_ref[...] - first
    points_copy.wait()
    for base in range(0, count, chunk):
        which = lax.broadcasted_iota(jnp.int32, (chunk, total), 0) + base
        hot = jnp.where(which == local_row, 1.0, 0.0).astype(jnp.bfloat16)
        picked = picked + contract(jnp.concatenate(split3(local_ref[:, base : base + chunk]), 0), hot, 1, 0)
    point = picked[:width] + picked[width : 2 * width] + picked[2 * width :]
    spare = rows_ref.shape[1] - rank - width
    rows_ref[:, rank:] = jnp.concatenate([point, jnp.zeros((spare, total), jnp.float32)], 0).T

    def wait(k, _):
        copy(0, 0).wait()
        return 0

    lax.fori_loop(0, started, wait, 0)
    mine = index & 1
    keep_ref[...] = rows_ref[pl.ds(pl.multiple_of(mine * half, 8), half), :]
    send_ref[...] = rows_ref[pl.ds(pl.multiple_of((1 - mine) * half, 8), half), :]


def pick_rows(points_t, factor, pivots):
    rank = factor.shape[1]
    total = pivots.shape[0]
    lanes = rank + -(-points_t.shape[0] // 128) * 128
    vmem = pl.BlockSpec(memory_space=pltpu.VMEM)
    anywhere = pl.BlockSpec(memory_space=pl.ANY)
    return pl.pallas_call(
        pick_kernel,
        in_specs=[pl.BlockSpec(memory_space=pltpu.SMEM), vmem, anywhere, anywhere],
        out_specs=[vmem, vmem],
        out_shape=[near_by(total // 2, lanes)] * 2,
        scratch_shapes=[
            pltpu.VMEM((total, lanes), jnp.float32),
            pltpu.VMEM(points_t.shape, jnp.float32),
            pltpu.SemaphoreType.DMA,
            pltpu.SemaphoreType.DMA,
        ],
        compiler_params=pltpu.CompilerParams(vmem_limit_bytes=vmem_bytes),
        name="pick_rows",
    )(pivots, pltpu.with_memory_space_constraint(pivots[None], pltpu.HBM), points_t, factor)


def residual_kernel(
    points_ref,
    factor_ref,
    mine_ref,
    other_ref,
    res_ref,
    keep_ref,
    send_ref,
    pivot_ref,
    sum_ref,
    wide,
    last,
    high,
    low,
    norm,
):
    width = points_ref.shape[0]
    rank = factor_ref.shape[1]

    @pl.when(pl.program_id(0) == 0)
    def _():
        join(pivot_ref, mine_ref, other_ref)
        p = pivot_ref[:, rank : rank + width]
        norm[...] = contract(jnp.ones((8, width), jnp.float32), p * p, 1, 1, highest)
        a, b, c = split3(-2.0 * p)
        one = jnp.ones(a.shape, jnp.bfloat16)
        wide[...] = jnp.concatenate([a, a, b, b], 1)
        last[...] = jnp.concatenate([c, a, one, one], 1)
        high[...], low[...] = split2(pivot_ref[:, :rank])
        sum_ref[...] = jnp.zeros_like(sum_ref)

    x = points_ref[...]
    a, b, c = split3(x)
    sq = jnp.sum(x * x, 0, keepdims=True)
    n1, n2, n3 = split3(sq)
    row = lax.broadcasted_iota(jnp.int32, (2 * width, x.shape[1]), 0)
    zero = jnp.zeros((), jnp.bfloat16)
    norms = jnp.where(row == 0, n1, jnp.where(row == 1, n2, jnp.where(row == 2, n3, zero)))
    dist = contract(jnp.concatenate([a, b, a, b], 0), wide[...], 0, 1)
    dist = dist + contract(jnp.concatenate([a, c, norms], 0), last[...], 0, 1)
    dist = dist + norm[0:1, :]
    kern = jnp.exp(-dist / width)
    fh, fl = split2(factor_ref[...])
    qh = high[...]
    res = kern - (contract(fh, qh, 1, 1) + (contract(fh, low[...], 1, 1) + contract(fl, qh, 1, 1)))
    res_ref[...] = res
    rh, rl = split2(res)
    sum_ref[:, :rank] += contract(rh, fh, 0, 0) + (contract(rh, fl, 0, 0) + contract(rl, fh, 0, 0))
    sum_ref[:, rank:] += contract(rh, rh, 0, 0) + (contract(rh, rl, 0, 0) + contract(rl, rh, 0, 0))

    @pl.when(pl.program_id(0) == pl.num_programs(0) - 1)
    def _():
        half = sum_ref.shape[0] // 2
        mine = position() & 1
        keep_ref[...] = sum_ref[pl.ds(pl.multiple_of(mine * half, 8), half), :]
        send_ref[...] = sum_ref[pl.ds(pl.multiple_of((1 - mine) * half, 8), half), :]


def residuals(points_t, factor, mine, other):
    width, count = points_t.shape
    rank = factor.shape[1]
    half, lanes = mine.shape
    total = 2 * half
    tile = min(1024, count)
    bf16 = jnp.bfloat16
    return pl.pallas_call(
        residual_kernel,
        grid=(count // tile,),
        in_specs=[
            pl.BlockSpec((width, tile), lambda i: (0, i)),
            pl.BlockSpec((tile, rank), lambda i: (i, 0)),
            pl.BlockSpec((half, lanes), lambda i: (0, 0)),
            pl.BlockSpec((half, lanes), lambda i: (0, 0)),
        ],
        out_specs=[
            pl.BlockSpec((tile, total), lambda i: (i, 0)),
            pl.BlockSpec((half, rank + total), lambda i: (0, 0)),
            pl.BlockSpec((half, rank + total), lambda i: (0, 0)),
            pl.BlockSpec((total, lanes), lambda i: (0, 0)),
        ],
        out_shape=[
            near_by(count, total),
            near_by(half, rank + total),
            near_by(half, rank + total),
            near_by(total, lanes),
        ],
        scratch_shapes=[
            pltpu.VMEM((total, rank + total), jnp.float32),
            pltpu.VMEM((total, 4 * width), bf16),
            pltpu.VMEM((total, 4 * width), bf16),
            pltpu.VMEM((total, rank), bf16),
            pltpu.VMEM((total, rank), bf16),
            pltpu.VMEM((8, total), jnp.float32),
        ],
        compiler_params=pltpu.CompilerParams(vmem_limit_bytes=vmem_bytes),
        name="residuals",
    )(points_t, factor, mine, other)


def eliminate(work, size, begin, end):
    step = panel_rows
    for start in range(begin, end, step):
        after = start + step
        panel = work[start:after, :]
        rows = lax.broadcasted_iota(jnp.int32, (step, size), 0)
        cols = [jnp.broadcast_to(panel[:, start + k : start + k + 1], (step, size)) for k in range(step)]
        left = panel[:, :size]
        right = panel[:, size:]
        scale = jnp.zeros((step, size), jnp.float32)
        solved = jnp.zeros((step, size), jnp.float32)
        for j in range(step):
            here = rows == j
            root = lax.rsqrt(jnp.broadcast_to(cols[j][j : j + 1], (step, size)))
            inv = root * root
            mult = jnp.where(here, 0.0, cols[j] * inv)
            scale = jnp.where(here, inv, scale)
            pivot_right = jnp.broadcast_to(right[j : j + 1], (step, size))
            solved = jnp.where(here, pivot_right * root, solved)
            for k in range(j + 1, step):
                cols[k] = cols[k] - mult * jnp.broadcast_to(cols[k][j : j + 1], (step, size))
            left = left - mult * jnp.broadcast_to(left[j : j + 1], (step, size))
            right = right - mult * pivot_right
        work[start:after, size:] = solved
        if after < size:
            parts = split3(jnp.concatenate([left * scale, right * scale], 1))
            above = [jnp.zeros((start, 2 * size), jnp.bfloat16)] if start else []
            below = [jnp.zeros((size - after, 2 * size), jnp.bfloat16)]
            e1, e2, e3 = [jnp.concatenate(above + [part] + below, 0) for part in parts]
            a1, a2, a3 = split3(work[after:, :size])
            update = contract(a1, e1, 1, 0) + (contract(a1, e2, 1, 0) + contract(a2, e1, 1, 0))
            update = update + (contract(a1, e3, 1, 0) + contract(a2, e2, 1, 0) + contract(a3, e1, 1, 0))
            work[after:, :] = work[after:, :] - update


def pairs_kernel(width, pivot_ref, kern_ref, outer_ref):
    rank = pivot_ref.shape[1] - -(-width // 128) * 128
    p = pivot_ref[:, rank : rank + width]
    q = pivot_ref[:, :rank]
    sq = p * p
    norm_row = contract(jnp.ones((8, width), jnp.float32), sq, 1, 1, highest)[0:1]
    norm_col = jnp.sum(sq, 1, keepdims=True)
    kern_ref[...] = jnp.exp(-(norm_col + norm_row - 2.0 * contract(p, p, 1, 1, highest)) / width)
    outer_ref[...] = contract(q, q, 1, 1, highest)


def pivot_pairs(fetched, width):
    total = fetched.shape[0]
    return pl.pallas_call(
        functools.partial(pairs_kernel, width),
        out_shape=[near_by(total, total)] * 2,
        compiler_params=pltpu.CompilerParams(vmem_limit_bytes=vmem_bytes),
        name="pivot_pairs",
    )(fetched)


def set_up(work, kern_ref, block, begin, size):
    end = begin + size
    eye = jnp.where(
        lax.broadcasted_iota(jnp.int32, (size, size), 0) == lax.broadcasted_iota(jnp.int32, (size, size), 1), 1.0, 0.0
    )
    shift = nugget + jnp.max(jnp.sum(jnp.abs(block), 1, keepdims=True), axis=0, keepdims=True)
    work[:, :size] = kern_ref[begin:end, begin:end] - block + shift * eye
    work[:, size:] = eye


def first_kernel(size, kern_ref, outer_ref, inv_ref, work):
    set_up(work, kern_ref, outer_ref[:size, :size], 0, size)
    eliminate(work, size, 0, size)
    inv_ref[...] = work[:, size:]


def first_block(kern, outer, size):
    return pl.pallas_call(
        functools.partial(first_kernel, size),
        out_shape=near_by(size, size),
        scratch_shapes=[pltpu.VMEM((size, 2 * size), jnp.float32)],
        compiler_params=pltpu.CompilerParams(vmem_limit_bytes=vmem_bytes),
        name="first_block",
    )(kern, outer)


def open_kernel(begin, size, rows, kern_ref, outer_ref, before_ref, work_ref, mixed_ref):
    end = begin + size
    mixed = contract(kern_ref[begin:end, :begin] - outer_ref[begin:end, :begin], before_ref[...], 1, 1, highest)
    mixed_ref[...] = mixed
    block = outer_ref[begin:end, begin:end] + contract(mixed, mixed, 1, 1, highest)
    set_up(work_ref, kern_ref, block, begin, size)
    eliminate(work_ref, size, 0, rows)


def open_block(kern, outer, before, begin, size, rows):
    return pl.pallas_call(
        functools.partial(open_kernel, begin, size, rows),
        out_shape=[near_by(size, 2 * size), near_by(size, begin)],
        compiler_params=pltpu.CompilerParams(vmem_limit_bytes=vmem_bytes),
        name="open_block",
    )(kern, outer, before)


def close_kernel(begin, size, rows, done_ref, mixed_ref, before_ref, inv_ref, work):
    work[...] = done_ref[...]
    eliminate(work, size, rows, size)
    inverse = work[:, size:]
    before = before_ref[...]
    inv_ref[:begin, :begin] = before
    inv_ref[:begin, begin:] = jnp.zeros((begin, size), jnp.float32)
    inv_ref[begin:, begin:] = inverse
    inv_ref[begin:, :begin] = -contract(inverse, contract(mixed_ref[...], before, 1, 0, highest), 1, 0, highest)


def close_block(done, mixed, before, begin, size, rows):
    end = begin + size
    return pl.pallas_call(
        functools.partial(close_kernel, begin, size, rows),
        out_shape=near_by(end, end),
        scratch_shapes=[pltpu.VMEM((size, 2 * size), jnp.float32)],
        compiler_params=pltpu.CompilerParams(vmem_limit_bytes=vmem_bytes),
        name="close_block",
    )(done, mixed, before)


def columns_kernel(res_ref, inv_ref, *refs):
    out_ref, one, two, three = refs[-4:]

    @pl.when(pl.program_id(0) == 0)
    def _():
        one[...], two[...], three[...] = split3(inv_ref[...])

    a, b, c = split3(res_ref[...])
    out = contract(a, one[...], 1, 1) + (contract(a, two[...], 1, 1) + contract(b, one[...], 1, 1))
    out_ref[...] = out + (contract(b, two[...], 1, 1) + contract(a, three[...], 1, 1) + contract(c, one[...], 1, 1))


def new_columns(res, inv, made, tile, begin, end):
    count, total = res.shape
    in_specs = [
        pl.BlockSpec((tile, total), lambda i: (i + begin, 0)),
        pl.BlockSpec((total, total), lambda i: (0, 0)),
    ]
    args = (res, inv)
    if made is not None:
        in_specs.append(pl.BlockSpec(memory_space=pl.ANY))
        args = (res, inv, made)
    return pl.pallas_call(
        columns_kernel,
        grid=(end - begin,),
        in_specs=in_specs,
        out_specs=pl.BlockSpec((tile, total), lambda i: (i + begin, 0)),
        out_shape=jax.ShapeDtypeStruct((count, total), jnp.float32),
        scratch_shapes=[pltpu.VMEM((total, total), jnp.bfloat16)] * 3,
        input_output_aliases={} if made is None else {2: 0},
        compiler_params=pltpu.CompilerParams(vmem_limit_bytes=vmem_bytes),
        name="new_columns",
    )(*args)


def gram_kernel(count, mine_ref, other_ref, inv_ref, out_ref, sum_ref):
    join(sum_ref, mine_ref, other_ref)
    inv = inv_ref[...]
    rank = sum_ref.shape[1] - inv.shape[0]
    half = contract(inv, sum_ref[...], 1, 0, highest)
    out_ref[:, :rank] = half[:, :rank] / count
    out_ref[:, rank:] = contract(half[:, rank:], inv, 1, 1, highest) / count


def gram_rows(mine, other, inv, count):
    half, lanes = mine.shape
    return pl.pallas_call(
        functools.partial(gram_kernel, count),
        out_shape=jax.ShapeDtypeStruct((2 * half, lanes), jnp.float32),
        scratch_shapes=[pltpu.VMEM((2 * half, lanes), jnp.float32)],
        compiler_params=pltpu.CompilerParams(vmem_limit_bytes=vmem_bytes),
        name="gram_rows",
    )(mine, other, inv)


def sum_over_devices(keep, send, index, bits, work=None):
    def swap(piece, mask):
        pairs = [(i, i ^ mask) for i in range(1 << bits)]
        if work is None or not work.steps:
            return lax.ppermute(piece, AXES, pairs)
        piece, work.state = lax.optimization_barrier((piece, work.state))
        got = lax.ppermute(piece, AXES, pairs)
        work.run()
        got, work.state = lax.optimization_barrier((got, work.state))
        return got

    near = min(halvings, bits)
    x = keep + swap(send, 1)
    for bit in range(1, near):
        half = x.shape[0] // 2
        mine = (index >> bit) & 1
        sent = lax.dynamic_slice_in_dim(x, (1 - mine) * half, half, 0)
        x = lax.dynamic_slice_in_dim(x, mine * half, half, 0) + swap(sent, 1 << bit)
    for bit in range(near, bits):
        x = x + swap(x, 1 << bit)
    for bit in reversed(range(1, near)):
        mine = (index >> bit) & 1
        other = swap(x, 1 << bit)
        x = jnp.concatenate([jnp.where(mine == 0, x, other), jnp.where(mine == 0, other, x)], 0)
    return x, swap(x, 1)


class Work:
    def __init__(self, state, steps):
        self.state = state
        self.steps = list(steps)

    def run(self):
        self.state = self.steps.pop(0)(self.state)


def body(bits, points, factor, pivots):
    count, width = points.shape
    blocks, size = pivots.shape
    index = position()
    points_t = pltpu.with_memory_space_constraint(points.T, pltpu.HBM)
    factor = pltpu.with_memory_space_constraint(factor, pltpu.HBM)
    fetched = sum_over_devices(*pick_rows(points_t, factor, pivots.reshape(-1)), index, bits)
    res, keep, send, pivot_rows = residuals(points_t, factor, *fetched)

    def pairs(state):
        return dict(state, pairs=pivot_pairs(state.pop("rows"), width))

    def first(state):
        return dict(state, inv=first_block(*state["pairs"], size))

    def open_next(begin):
        def run(state):
            return dict(state, open=open_block(*state["pairs"], state["inv"], begin, size, size // 2))

        return run

    def close_next(begin):
        def run(state):
            done, mixed = state.pop("open")
            return dict(state, inv=close_block(done, mixed, state["inv"], begin, size, size // 2))

        return run

    tile = min(1024, count)
    tiles = count // tile
    cuts = [0, tiles // 4, tiles // 2, tiles]

    def columns(begin, end):
        def run(state):
            return dict(state, made=new_columns(state["res"], state["inv"], state["made"], tile, begin, end))

        return run

    steps = [pairs, first]
    for begin in range(size, blocks * size, size):
        steps += [open_next(begin), close_next(begin)]
    steps += [columns(b, e) for b, e in zip(cuts, cuts[1:]) if e > b]
    work = Work({"rows": pivot_rows, "res": res, "made": None}, steps)
    total = sum_over_devices(keep, send, index, bits, work)
    while work.steps:
        work.run()
    return work.state["made"], gram_rows(*total, work.state["inv"], count)


def solution(mesh):
    bits = (mesh.size - 1).bit_length()
    assert mesh.size == 1 << bits
    in_specs = (P(AXES, None), P(AXES, None), P())
    out_specs = (P(AXES, None), P())
    return jax.shard_map(
        functools.partial(body, bits), mesh=mesh, in_specs=in_specs, out_specs=out_specs, check_vma=False
    )
```

```python
import functools

import jax
import jax.numpy as jnp
from jax import lax
from jax.experimental import pallas as pl
from jax.experimental.pallas import tpu as pltpu
from jax.sharding import PartitionSpec as P

AXES = ("row", "col")
nugget = 0.1
highest = lax.Precision.HIGHEST
panel_rows = 16
vmem_bytes = 32 << 20


def split2(x):
    a = x.astype(jnp.bfloat16)
    return a, (x - a.astype(jnp.float32)).astype(jnp.bfloat16)


def split3(x):
    a = x.astype(jnp.bfloat16)
    rest = x - a.astype(jnp.float32)
    b = rest.astype(jnp.bfloat16)
    return a, b, (rest - b.astype(jnp.float32)).astype(jnp.bfloat16)


def near_by(*shape):
    return pltpu.VMEM(shape, jnp.float32)


def position():
    return lax.axis_index("row") * lax.axis_size("col") + lax.axis_index("col")


def join(out_ref, mine_ref, other_ref):
    half = mine_ref.shape[0]
    mine = position() & 1
    out_ref[pl.ds(pl.multiple_of(mine * half, 8), half), :] = mine_ref[...]
    out_ref[pl.ds(pl.multiple_of((1 - mine) * half, 8), half), :] = other_ref[...]


def contract(x, y, dim_x, dim_y, precision=None):
    return lax.dot_general(
        x, y, (((dim_x,), (dim_y,)), ((), ())), precision=precision, preferred_element_type=jnp.float32
    )


def pick_kernel(
    pivots_ref, pivots_row_ref, points_ref, factor_ref, keep_ref, send_ref, rows_ref, local_ref, sem, points_sem
):
    width, count = points_ref.shape
    rank = factor_ref.shape[1]
    total = rows_ref.shape[0]
    half = total // 2
    index = position()
    first = index * count
    points_copy = pltpu.make_async_copy(points_ref, local_ref, points_sem)
    points_copy.start()
    rows_ref[:, :rank] = jnp.zeros((total, rank), jnp.float32)

    def copy(row, k):
        return pltpu.make_async_copy(factor_ref.at[pl.ds(row, 1), :], rows_ref.at[pl.ds(k, 1), pl.ds(0, rank)], sem)

    def start(k, started):
        local = pivots_ref[k] - first
        inside = (local >= 0) & (local < count)

        @pl.when(inside)
        def _():
            copy(local, k).start()

        return started + inside.astype(jnp.int32)

    started = lax.fori_loop(0, total, start, 0, unroll=8)
    chunk = min(512, count)
    picked = jnp.zeros((3 * width, total), jnp.float32)
    local_row = pivots_row_ref[...] - first
    points_copy.wait()
    for base in range(0, count, chunk):
        which = lax.broadcasted_iota(jnp.int32, (chunk, total), 0) + base
        hot = jnp.where(which == local_row, 1.0, 0.0).astype(jnp.bfloat16)
        picked = picked + contract(jnp.concatenate(split3(local_ref[:, base : base + chunk]), 0), hot, 1, 0)
    point = picked[:width] + picked[width : 2 * width] + picked[2 * width :]
    spare = rows_ref.shape[1] - rank - width
    rows_ref[:, rank:] = jnp.concatenate([point, jnp.zeros((spare, total), jnp.float32)], 0).T

    def wait(k, _):
        copy(0, 0).wait()
        return 0

    lax.fori_loop(0, started, wait, 0)
    mine = index & 1
    keep_ref[...] = rows_ref[pl.ds(pl.multiple_of(mine * half, 8), half), :]
    send_ref[...] = rows_ref[pl.ds(pl.multiple_of((1 - mine) * half, 8), half), :]


def pick_rows(points_t, factor, pivots):
    rank = factor.shape[1]
    total = pivots.shape[0]
    lanes = rank + -(-points_t.shape[0] // 128) * 128
    vmem = pl.BlockSpec(memory_space=pltpu.VMEM)
    anywhere = pl.BlockSpec(memory_space=pl.ANY)
    return pl.pallas_call(
        pick_kernel,
        in_specs=[pl.BlockSpec(memory_space=pltpu.SMEM), vmem, anywhere, anywhere],
        out_specs=[vmem, vmem],
        out_shape=[near_by(total // 2, lanes)] * 2,
        scratch_shapes=[
            pltpu.VMEM((total, lanes), jnp.float32),
            pltpu.VMEM(points_t.shape, jnp.float32),
            pltpu.SemaphoreType.DMA,
            pltpu.SemaphoreType.DMA,
        ],
        compiler_params=pltpu.CompilerParams(vmem_limit_bytes=vmem_bytes),
        name="pick_rows",
    )(pivots, pltpu.with_memory_space_constraint(pivots[None], pltpu.HBM), points_t, factor)


def residual_kernel(
    points_ref,
    factor_ref,
    mine_ref,
    other_ref,
    res_ref,
    keep_ref,
    send_ref,
    pivot_ref,
    sum_ref,
    wide,
    last,
    high,
    low,
    norm,
):
    width = points_ref.shape[0]
    rank = factor_ref.shape[1]

    @pl.when(pl.program_id(0) == 0)
    def _():
        join(pivot_ref, mine_ref, other_ref)
        p = pivot_ref[:, rank : rank + width]
        norm[...] = contract(jnp.ones((8, width), jnp.float32), p * p, 1, 1, highest)
        a, b, c = split3(-2.0 * p)
        one = jnp.ones(a.shape, jnp.bfloat16)
        wide[...] = jnp.concatenate([a, a, b, b], 1)
        last[...] = jnp.concatenate([c, a, one, one], 1)
        high[...], low[...] = split2(pivot_ref[:, :rank])
        sum_ref[...] = jnp.zeros_like(sum_ref)

    x = points_ref[...]
    a, b, c = split3(x)
    sq = jnp.sum(x * x, 0, keepdims=True)
    n1, n2, n3 = split3(sq)
    row = lax.broadcasted_iota(jnp.int32, (2 * width, x.shape[1]), 0)
    zero = jnp.zeros((), jnp.bfloat16)
    norms = jnp.where(row == 0, n1, jnp.where(row == 1, n2, jnp.where(row == 2, n3, zero)))
    dist = contract(jnp.concatenate([a, b, a, b], 0), wide[...], 0, 1)
    dist = dist + contract(jnp.concatenate([a, c, norms], 0), last[...], 0, 1)
    dist = dist + norm[0:1, :]
    kern = jnp.exp(-dist / width)
    fh, fl = split2(factor_ref[...])
    qh = high[...]
    res = kern - (contract(fh, qh, 1, 1) + (contract(fh, low[...], 1, 1) + contract(fl, qh, 1, 1)))
    res_ref[...] = res
    rh, rl = split2(res)
    sum_ref[:, :rank] += contract(rh, fh, 0, 0) + (contract(rh, fl, 0, 0) + contract(rl, fh, 0, 0))
    sum_ref[:, rank:] += contract(rh, rh, 0, 0) + (contract(rh, rl, 0, 0) + contract(rl, rh, 0, 0))

    @pl.when(pl.program_id(0) == pl.num_programs(0) - 1)
    def _():
        half = sum_ref.shape[0] // 2
        mine = position() & 1
        keep_ref[...] = sum_ref[pl.ds(pl.multiple_of(mine * half, 8), half), :]
        send_ref[...] = sum_ref[pl.ds(pl.multiple_of((1 - mine) * half, 8), half), :]


def residuals(points_t, factor, mine, other):
    width, count = points_t.shape
    rank = factor.shape[1]
    half, lanes = mine.shape
    total = 2 * half
    tile = min(1024, count)
    bf16 = jnp.bfloat16
    return pl.pallas_call(
        residual_kernel,
        grid=(count // tile,),
        in_specs=[
            pl.BlockSpec((width, tile), lambda i: (0, i)),
            pl.BlockSpec((tile, rank), lambda i: (i, 0)),
            pl.BlockSpec((half, lanes), lambda i: (0, 0)),
            pl.BlockSpec((half, lanes), lambda i: (0, 0)),
        ],
        out_specs=[
            pl.BlockSpec((tile, total), lambda i: (i, 0)),
            pl.BlockSpec((half, rank + total), lambda i: (0, 0)),
            pl.BlockSpec((half, rank + total), lambda i: (0, 0)),
            pl.BlockSpec((total, lanes), lambda i: (0, 0)),
        ],
        out_shape=[
            near_by(count, total),
            near_by(half, rank + total),
            near_by(half, rank + total),
            near_by(total, lanes),
        ],
        scratch_shapes=[
            pltpu.VMEM((total, rank + total), jnp.float32),
            pltpu.VMEM((total, 4 * width), bf16),
            pltpu.VMEM((total, 4 * width), bf16),
            pltpu.VMEM((total, rank), bf16),
            pltpu.VMEM((total, rank), bf16),
            pltpu.VMEM((8, total), jnp.float32),
        ],
        compiler_params=pltpu.CompilerParams(vmem_limit_bytes=vmem_bytes),
        name="residuals",
    )(points_t, factor, mine, other)


def eliminate(work, size, begin, end):
    step = panel_rows
    for start in range(begin, end, step):
        after = start + step
        panel = work[start:after, :]
        rows = lax.broadcasted_iota(jnp.int32, (step, size), 0)
        cols = [jnp.broadcast_to(panel[:, start + k : start + k + 1], (step, size)) for k in range(step)]
        left = panel[:, :size]
        right = panel[:, size:]
        scale = jnp.zeros((step, size), jnp.float32)
        solved = jnp.zeros((step, size), jnp.float32)
        for j in range(step):
            here = rows == j
            root = lax.rsqrt(jnp.broadcast_to(cols[j][j : j + 1], (step, size)))
            inv = root * root
            mult = jnp.where(here, 0.0, cols[j] * inv)
            scale = jnp.where(here, inv, scale)
            pivot_right = jnp.broadcast_to(right[j : j + 1], (step, size))
            solved = jnp.where(here, pivot_right * root, solved)
            for k in range(j + 1, step):
                cols[k] = cols[k] - mult * jnp.broadcast_to(cols[k][j : j + 1], (step, size))
            left = left - mult * jnp.broadcast_to(left[j : j + 1], (step, size))
            right = right - mult * pivot_right
        work[start:after, size:] = solved
        if after < size:
            parts = split3(jnp.concatenate([left * scale, right * scale], 1))
            above = [jnp.zeros((start, 2 * size), jnp.bfloat16)] if start else []
            below = [jnp.zeros((size - after, 2 * size), jnp.bfloat16)]
            e1, e2, e3 = [jnp.concatenate(above + [part] + below, 0) for part in parts]
            a1, a2, a3 = split3(work[after:, :size])
            update = contract(a1, e1, 1, 0) + (contract(a1, e2, 1, 0) + contract(a2, e1, 1, 0))
            update = update + (contract(a1, e3, 1, 0) + contract(a2, e2, 1, 0) + contract(a3, e1, 1, 0))
            work[after:, :] = work[after:, :] - update


def pairs_kernel(width, pivot_ref, kern_ref, outer_ref):
    rank = pivot_ref.shape[1] - -(-width // 128) * 128
    p = pivot_ref[:, rank : rank + width]
    q = pivot_ref[:, :rank]
    sq = p * p
    norm_row = contract(jnp.ones((8, width), jnp.float32), sq, 1, 1, highest)[0:1]
    norm_col = jnp.sum(sq, 1, keepdims=True)
    kern_ref[...] = jnp.exp(-(norm_col + norm_row - 2.0 * contract(p, p, 1, 1, highest)) / width)
    outer_ref[...] = contract(q, q, 1, 1, highest)


def pivot_pairs(fetched, width):
    total = fetched.shape[0]
    return pl.pallas_call(
        functools.partial(pairs_kernel, width),
        out_shape=[near_by(total, total)] * 2,
        compiler_params=pltpu.CompilerParams(vmem_limit_bytes=vmem_bytes),
        name="pivot_pairs",
    )(fetched)


def set_up(work, kern_ref, block, begin, size):
    end = begin + size
    eye = jnp.where(
        lax.broadcasted_iota(jnp.int32, (size, size), 0) == lax.broadcasted_iota(jnp.int32, (size, size), 1), 1.0, 0.0
    )
    shift = nugget + jnp.max(jnp.sum(jnp.abs(block), 1, keepdims=True), axis=0, keepdims=True)
    work[:, :size] = kern_ref[begin:end, begin:end] - block + shift * eye
    work[:, size:] = eye


def first_kernel(size, kern_ref, outer_ref, inv_ref, work):
    set_up(work, kern_ref, outer_ref[:size, :size], 0, size)
    eliminate(work, size, 0, size)
    inv_ref[...] = work[:, size:]


def first_block(kern, outer, size):
    return pl.pallas_call(
        functools.partial(first_kernel, size),
        out_shape=near_by(size, size),
        scratch_shapes=[pltpu.VMEM((size, 2 * size), jnp.float32)],
        compiler_params=pltpu.CompilerParams(vmem_limit_bytes=vmem_bytes),
        name="first_block",
    )(kern, outer)


def open_kernel(begin, size, rows, kern_ref, outer_ref, before_ref, work_ref, mixed_ref):
    end = begin + size
    mixed = contract(kern_ref[begin:end, :begin] - outer_ref[begin:end, :begin], before_ref[...], 1, 1, highest)
    mixed_ref[...] = mixed
    block = outer_ref[begin:end, begin:end] + contract(mixed, mixed, 1, 1, highest)
    set_up(work_ref, kern_ref, block, begin, size)
    eliminate(work_ref, size, 0, rows)


def open_block(kern, outer, before, begin, size, rows):
    return pl.pallas_call(
        functools.partial(open_kernel, begin, size, rows),
        out_shape=[near_by(size, 2 * size), near_by(size, begin)],
        compiler_params=pltpu.CompilerParams(vmem_limit_bytes=vmem_bytes),
        name="open_block",
    )(kern, outer, before)


def close_kernel(begin, size, rows, done_ref, mixed_ref, before_ref, inv_ref, work):
    work[...] = done_ref[...]
    eliminate(work, size, rows, size)
    inverse = work[:, size:]
    before = before_ref[...]
    inv_ref[:begin, :begin] = before
    inv_ref[:begin, begin:] = jnp.zeros((begin, size), jnp.float32)
    inv_ref[begin:, begin:] = inverse
    inv_ref[begin:, :begin] = -contract(inverse, contract(mixed_ref[...], before, 1, 0, highest), 1, 0, highest)


def close_block(done, mixed, before, begin, size, rows):
    end = begin + size
    return pl.pallas_call(
        functools.partial(close_kernel, begin, size, rows),
        out_shape=near_by(end, end),
        scratch_shapes=[pltpu.VMEM((size, 2 * size), jnp.float32)],
        compiler_params=pltpu.CompilerParams(vmem_limit_bytes=vmem_bytes),
        name="close_block",
    )(done, mixed, before)


def columns_kernel(res_ref, inv_ref, *refs):
    out_ref, one, two, three = refs[-4:]

    @pl.when(pl.program_id(0) == 0)
    def _():
        one[...], two[...], three[...] = split3(inv_ref[...])

    a, b, c = split3(res_ref[...])
    out = contract(a, one[...], 1, 1) + (contract(a, two[...], 1, 1) + contract(b, one[...], 1, 1))
    out_ref[...] = out + (contract(b, two[...], 1, 1) + contract(a, three[...], 1, 1) + contract(c, one[...], 1, 1))


def new_columns(res, inv, made, tile, begin, end):
    count, total = res.shape
    in_specs = [
        pl.BlockSpec((tile, total), lambda i: (i + begin, 0)),
        pl.BlockSpec((total, total), lambda i: (0, 0)),
    ]
    args = (res, inv)
    if made is not None:
        in_specs.append(pl.BlockSpec(memory_space=pl.ANY))
        args = (res, inv, made)
    return pl.pallas_call(
        columns_kernel,
        grid=(end - begin,),
        in_specs=in_specs,
        out_specs=pl.BlockSpec((tile, total), lambda i: (i + begin, 0)),
        out_shape=jax.ShapeDtypeStruct((count, total), jnp.float32),
        scratch_shapes=[pltpu.VMEM((total, total), jnp.bfloat16)] * 3,
        input_output_aliases={} if made is None else {2: 0},
        compiler_params=pltpu.CompilerParams(vmem_limit_bytes=vmem_bytes),
        name="new_columns",
    )(*args)


def gram_kernel(count, mine_ref, other_ref, inv_ref, out_ref, sum_ref):
    join(sum_ref, mine_ref, other_ref)
    inv = inv_ref[...]
    rank = sum_ref.shape[1] - inv.shape[0]
    half = contract(inv, sum_ref[...], 1, 0, highest)
    out_ref[:, :rank] = half[:, :rank] / count
    out_ref[:, rank:] = contract(half[:, rank:], inv, 1, 1, highest) / count


def gram_rows(mine, other, inv, count):
    half, lanes = mine.shape
    return pl.pallas_call(
        functools.partial(gram_kernel, count),
        out_shape=jax.ShapeDtypeStruct((2 * half, lanes), jnp.float32),
        scratch_shapes=[pltpu.VMEM((2 * half, lanes), jnp.float32)],
        compiler_params=pltpu.CompilerParams(vmem_limit_bytes=vmem_bytes),
        name="gram_rows",
    )(mine, other, inv)


def sum_over_devices(keep, send, index, bits, work=None):
    def swap(pieces, masks):
        beside = work is not None and work.steps
        if beside:
            pieces, work.state = lax.optimization_barrier((pieces, work.state))
        got = [
            lax.ppermute(piece, AXES, [(i, i ^ mask) for i in range(1 << bits)]) for piece, mask in zip(pieces, masks)
        ]
        if beside:
            work.run()
            got, work.state = lax.optimization_barrier((got, work.state))
        return got

    four = [2, 4, 6]
    quarter = keep.shape[0] // 4
    place = (index >> 1) & 3
    x = keep + swap([send], [1])[0]
    parts = [lax.dynamic_slice_in_dim(x, (place ^ (mask >> 1)) * quarter, quarter, 0) for mask in four]
    x = lax.dynamic_slice_in_dim(x, place * quarter, quarter, 0)
    for got in swap(parts, four):
        x = x + got
    for bit in range(3, bits):
        x = x + swap([x], [1 << bit])[0]
    parts = [x] + swap([x] * 3, four)
    rows = []
    for spot in range(4):
        which = place ^ spot
        rows.append(jnp.where(which < 2, jnp.where(which == 0, parts[0], parts[1]), jnp.where(which == 2, parts[2], parts[3])))
    x = jnp.concatenate(rows, 0)
    return x, swap([x], [1])[0]


class Work:
    def __init__(self, state, steps):
        self.state = state
        self.steps = list(steps)

    def run(self):
        self.state = self.steps.pop(0)(self.state)


def body(bits, points, factor, pivots):
    count, width = points.shape
    blocks, size = pivots.shape
    index = position()
    points_t = pltpu.with_memory_space_constraint(points.T, pltpu.HBM)
    factor = pltpu.with_memory_space_constraint(factor, pltpu.HBM)
    fetched = sum_over_devices(*pick_rows(points_t, factor, pivots.reshape(-1)), index, bits)
    res, keep, send, pivot_rows = residuals(points_t, factor, *fetched)

    def pairs(state):
        return dict(state, pairs=pivot_pairs(state.pop("rows"), width))

    def first(state):
        return dict(state, inv=first_block(*state["pairs"], size))

    def open_next(begin):
        def run(state):
            return dict(state, open=open_block(*state["pairs"], state["inv"], begin, size, size // 2))

        return run

    def close_next(begin):
        def run(state):
            done, mixed = state.pop("open")
            return dict(state, inv=close_block(done, mixed, state["inv"], begin, size, size // 2))

        return run

    tile = min(1024, count)
    tiles = count // tile
    cuts = [0, tiles - tiles // 4, tiles]

    def columns(begin, end):
        def run(state):
            return dict(state, made=new_columns(state["res"], state["inv"], state["made"], tile, begin, end))

        return run

    steps = [pairs, first]
    for begin in range(size, blocks * size, size):
        steps += [open_next(begin), close_next(begin)]
    steps += [columns(b, e) for b, e in zip(cuts, cuts[1:]) if e > b]
    work = Work({"rows": pivot_rows, "res": res, "made": None}, steps)
    total = sum_over_devices(keep, send, index, bits, work)
    while work.steps:
        work.run()
    return work.state["made"], gram_rows(*total, work.state["inv"], count)


def solution(mesh):
    bits = (mesh.size - 1).bit_length()
    assert mesh.size == 1 << bits and bits >= 3
    in_specs = (P(AXES, None), P(AXES, None), P())
    out_specs = (P(AXES, None), P())
    return jax.shard_map(
        functools.partial(body, bits), mesh=mesh, in_specs=in_specs, out_specs=out_specs, check_vma=False
    )
```

```python
import functools

import jax
import jax.numpy as jnp
from jax import lax
from jax.experimental import pallas as pl
from jax.experimental.pallas import tpu as pltpu
from jax.sharding import PartitionSpec as P

AXES = ("row", "col")
nugget = 0.1
highest = lax.Precision.HIGHEST
panel_rows = 16
vmem_bytes = 32 << 20


def split2(x):
    a = x.astype(jnp.bfloat16)
    return a, (x - a.astype(jnp.float32)).astype(jnp.bfloat16)


def split3(x):
    a = x.astype(jnp.bfloat16)
    rest = x - a.astype(jnp.float32)
    b = rest.astype(jnp.bfloat16)
    return a, b, (rest - b.astype(jnp.float32)).astype(jnp.bfloat16)


def near_by(*shape):
    return pltpu.VMEM(shape, jnp.float32)


def position():
    return lax.axis_index("row") * lax.axis_size("col") + lax.axis_index("col")


def join(out_ref, mine_ref, other_ref):
    half = mine_ref.shape[0]
    mine = position() & 1
    out_ref[pl.ds(pl.multiple_of(mine * half, 8), half), :] = mine_ref[...]
    out_ref[pl.ds(pl.multiple_of((1 - mine) * half, 8), half), :] = other_ref[...]


def contract(x, y, dim_x, dim_y, precision=None):
    return lax.dot_general(
        x, y, (((dim_x,), (dim_y,)), ((), ())), precision=precision, preferred_element_type=jnp.float32
    )


def pick_kernel(
    pivots_ref, pivots_row_ref, points_ref, factor_ref, keep_ref, send_ref, rows_ref, local_ref, sem, points_sem
):
    width, count = points_ref.shape
    rank = factor_ref.shape[1]
    total = rows_ref.shape[0]
    half = total // 2
    index = position()
    first = index * count
    points_copy = pltpu.make_async_copy(points_ref, local_ref, points_sem)
    points_copy.start()
    rows_ref[:, :rank] = jnp.zeros((total, rank), jnp.float32)

    def copy(row, k):
        return pltpu.make_async_copy(factor_ref.at[pl.ds(row, 1), :], rows_ref.at[pl.ds(k, 1), pl.ds(0, rank)], sem)

    def start(k, started):
        local = pivots_ref[k] - first
        inside = (local >= 0) & (local < count)

        @pl.when(inside)
        def _():
            copy(local, k).start()

        return started + inside.astype(jnp.int32)

    started = lax.fori_loop(0, total, start, 0, unroll=8)
    chunk = min(512, count)
    picked = jnp.zeros((3 * width, total), jnp.float32)
    local_row = pivots_row_ref[...] - first
    points_copy.wait()
    for base in range(0, count, chunk):
        which = lax.broadcasted_iota(jnp.int32, (chunk, total), 0) + base
        hot = jnp.where(which == local_row, 1.0, 0.0).astype(jnp.bfloat16)
        picked = picked + contract(jnp.concatenate(split3(local_ref[:, base : base + chunk]), 0), hot, 1, 0)
    point = picked[:width] + picked[width : 2 * width] + picked[2 * width :]
    spare = rows_ref.shape[1] - rank - width
    rows_ref[:, rank:] = jnp.concatenate([point, jnp.zeros((spare, total), jnp.float32)], 0).T

    def wait(k, _):
        copy(0, 0).wait()
        return 0

    lax.fori_loop(0, started, wait, 0)
    mine = index & 1
    keep_ref[...] = rows_ref[pl.ds(pl.multiple_of(mine * half, 8), half), :]
    send_ref[...] = rows_ref[pl.ds(pl.multiple_of((1 - mine) * half, 8), half), :]


def pick_rows(points_t, factor, pivots):
    rank = factor.shape[1]
    total = pivots.shape[0]
    lanes = rank + -(-points_t.shape[0] // 128) * 128
    vmem = pl.BlockSpec(memory_space=pltpu.VMEM)
    anywhere = pl.BlockSpec(memory_space=pl.ANY)
    return pl.pallas_call(
        pick_kernel,
        in_specs=[pl.BlockSpec(memory_space=pltpu.SMEM), vmem, anywhere, anywhere],
        out_specs=[vmem, vmem],
        out_shape=[near_by(total // 2, lanes)] * 2,
        scratch_shapes=[
            pltpu.VMEM((total, lanes), jnp.float32),
            pltpu.VMEM(points_t.shape, jnp.float32),
            pltpu.SemaphoreType.DMA,
            pltpu.SemaphoreType.DMA,
        ],
        compiler_params=pltpu.CompilerParams(vmem_limit_bytes=vmem_bytes),
        name="pick_rows",
    )(pivots, pltpu.with_memory_space_constraint(pivots[None], pltpu.HBM), points_t, factor)


def residual_kernel(
    points_ref,
    factor_ref,
    mine_ref,
    other_ref,
    res_ref,
    keep_ref,
    send_ref,
    pivot_ref,
    sum_ref,
    wide,
    last,
    high,
    low,
    norm,
):
    width = points_ref.shape[0]
    rank = factor_ref.shape[1]

    @pl.when(pl.program_id(0) == 0)
    def _():
        join(pivot_ref, mine_ref, other_ref)
        p = pivot_ref[:, rank : rank + width]
        norm[...] = contract(jnp.ones((8, width), jnp.float32), p * p, 1, 1, highest)
        a, b, c = split3(-2.0 * p)
        one = jnp.ones(a.shape, jnp.bfloat16)
        wide[...] = jnp.concatenate([a, a, b, b], 1)
        last[...] = jnp.concatenate([c, a, one, one], 1)
        high[...], low[...] = split2(pivot_ref[:, :rank])
        sum_ref[...] = jnp.zeros_like(sum_ref)

    x = points_ref[...]
    a, b, c = split3(x)
    sq = jnp.sum(x * x, 0, keepdims=True)
    n1, n2, n3 = split3(sq)
    row = lax.broadcasted_iota(jnp.int32, (2 * width, x.shape[1]), 0)
    zero = jnp.zeros((), jnp.bfloat16)
    norms = jnp.where(row == 0, n1, jnp.where(row == 1, n2, jnp.where(row == 2, n3, zero)))
    dist = contract(jnp.concatenate([a, b, a, b], 0), wide[...], 0, 1)
    dist = dist + contract(jnp.concatenate([a, c, norms], 0), last[...], 0, 1)
    dist = dist + norm[0:1, :]
    kern = jnp.exp(-dist / width)
    fh, fl = split2(factor_ref[...])
    qh = high[...]
    res = kern - (contract(fh, qh, 1, 1) + (contract(fh, low[...], 1, 1) + contract(fl, qh, 1, 1)))
    res_ref[...] = res
    rh, rl = split2(res)
    sum_ref[:, :rank] += contract(rh, fh, 0, 0) + (contract(rh, fl, 0, 0) + contract(rl, fh, 0, 0))
    sum_ref[:, rank:] += contract(rh, rh, 0, 0) + (contract(rh, rl, 0, 0) + contract(rl, rh, 0, 0))

    @pl.when(pl.program_id(0) == pl.num_programs(0) - 1)
    def _():
        half = sum_ref.shape[0] // 2
        mine = position() & 1
        keep_ref[...] = sum_ref[pl.ds(pl.multiple_of(mine * half, 8), half), :]
        send_ref[...] = sum_ref[pl.ds(pl.multiple_of((1 - mine) * half, 8), half), :]


def residuals(points_t, factor, mine, other):
    width, count = points_t.shape
    rank = factor.shape[1]
    half, lanes = mine.shape
    total = 2 * half
    tile = min(2048, count)
    bf16 = jnp.bfloat16
    return pl.pallas_call(
        residual_kernel,
        grid=(count // tile,),
        in_specs=[
            pl.BlockSpec((width, tile), lambda i: (0, i)),
            pl.BlockSpec((tile, rank), lambda i: (i, 0)),
            pl.BlockSpec((half, lanes), lambda i: (0, 0)),
            pl.BlockSpec((half, lanes), lambda i: (0, 0)),
        ],
        out_specs=[
            pl.BlockSpec((tile, total), lambda i: (i, 0)),
            pl.BlockSpec((half, rank + total), lambda i: (0, 0)),
            pl.BlockSpec((half, rank + total), lambda i: (0, 0)),
            pl.BlockSpec((total, lanes), lambda i: (0, 0)),
        ],
        out_shape=[
            near_by(count, total),
            near_by(half, rank + total),
            near_by(half, rank + total),
            near_by(total, lanes),
        ],
        scratch_shapes=[
            pltpu.VMEM((total, rank + total), jnp.float32),
            pltpu.VMEM((total, 4 * width), bf16),
            pltpu.VMEM((total, 4 * width), bf16),
            pltpu.VMEM((total, rank), bf16),
            pltpu.VMEM((total, rank), bf16),
            pltpu.VMEM((8, total), jnp.float32),
        ],
        compiler_params=pltpu.CompilerParams(vmem_limit_bytes=vmem_bytes),
        name="residuals",
    )(points_t, factor, mine, other)


def eliminate(work, size, begin, end):
    step = panel_rows
    for start in range(begin, end, step):
        after = start + step
        panel = work[start:after, :]
        rows = lax.broadcasted_iota(jnp.int32, (step, size), 0)
        cols = [jnp.broadcast_to(panel[:, start + k : start + k + 1], (step, size)) for k in range(step)]
        left = panel[:, :size]
        right = panel[:, size:]
        scale = jnp.zeros((step, size), jnp.float32)
        solved = jnp.zeros((step, size), jnp.float32)
        for j in range(step):
            here = rows == j
            root = lax.rsqrt(jnp.broadcast_to(cols[j][j : j + 1], (step, size)))
            inv = root * root
            mult = jnp.where(here, 0.0, cols[j] * inv)
            scale = jnp.where(here, inv, scale)
            pivot_right = jnp.broadcast_to(right[j : j + 1], (step, size))
            solved = jnp.where(here, pivot_right * root, solved)
            for k in range(j + 1, step):
                cols[k] = cols[k] - mult * jnp.broadcast_to(cols[k][j : j + 1], (step, size))
            left = left - mult * jnp.broadcast_to(left[j : j + 1], (step, size))
            right = right - mult * pivot_right
        work[start:after, size:] = solved
        if after < size:
            parts = split3(jnp.concatenate([left * scale, right * scale], 1))
            above = [jnp.zeros((start, 2 * size), jnp.bfloat16)] if start else []
            below = [jnp.zeros((size - after, 2 * size), jnp.bfloat16)]
            e1, e2, e3 = [jnp.concatenate(above + [part] + below, 0) for part in parts]
            a1, a2, a3 = split3(work[after:, :size])
            update = contract(a1, e1, 1, 0) + (contract(a1, e2, 1, 0) + contract(a2, e1, 1, 0))
            update = update + (contract(a1, e3, 1, 0) + contract(a2, e2, 1, 0) + contract(a3, e1, 1, 0))
            work[after:, :] = work[after:, :] - update


def pairs_kernel(width, pivot_ref, kern_ref, outer_ref):
    rank = pivot_ref.shape[1] - -(-width // 128) * 128
    p = pivot_ref[:, rank : rank + width]
    q = pivot_ref[:, :rank]
    sq = p * p
    norm_row = contract(jnp.ones((8, width), jnp.float32), sq, 1, 1, highest)[0:1]
    norm_col = jnp.sum(sq, 1, keepdims=True)
    kern_ref[...] = jnp.exp(-(norm_col + norm_row - 2.0 * contract(p, p, 1, 1, highest)) / width)
    outer_ref[...] = contract(q, q, 1, 1, highest)


def pivot_pairs(fetched, width):
    total = fetched.shape[0]
    return pl.pallas_call(
        functools.partial(pairs_kernel, width),
        out_shape=[near_by(total, total)] * 2,
        compiler_params=pltpu.CompilerParams(vmem_limit_bytes=vmem_bytes),
        name="pivot_pairs",
    )(fetched)


def set_up(work, kern_ref, block, begin, size):
    end = begin + size
    eye = jnp.where(
        lax.broadcasted_iota(jnp.int32, (size, size), 0) == lax.broadcasted_iota(jnp.int32, (size, size), 1), 1.0, 0.0
    )
    shift = nugget + jnp.max(jnp.sum(jnp.abs(block), 1, keepdims=True), axis=0, keepdims=True)
    work[:, :size] = kern_ref[begin:end, begin:end] - block + shift * eye
    work[:, size:] = eye


def first_kernel(size, kern_ref, outer_ref, inv_ref, work):
    set_up(work, kern_ref, outer_ref[:size, :size], 0, size)
    eliminate(work, size, 0, size)
    inv_ref[...] = work[:, size:]


def first_block(kern, outer, size):
    return pl.pallas_call(
        functools.partial(first_kernel, size),
        out_shape=near_by(size, size),
        scratch_shapes=[pltpu.VMEM((size, 2 * size), jnp.float32)],
        compiler_params=pltpu.CompilerParams(vmem_limit_bytes=vmem_bytes),
        name="first_block",
    )(kern, outer)


def open_kernel(begin, size, rows, kern_ref, outer_ref, before_ref, work_ref, mixed_ref):
    end = begin + size
    mixed = contract(kern_ref[begin:end, :begin] - outer_ref[begin:end, :begin], before_ref[...], 1, 1, highest)
    mixed_ref[...] = mixed
    block = outer_ref[begin:end, begin:end] + contract(mixed, mixed, 1, 1, highest)
    set_up(work_ref, kern_ref, block, begin, size)
    eliminate(work_ref, size, 0, rows)


def open_block(kern, outer, before, begin, size, rows):
    return pl.pallas_call(
        functools.partial(open_kernel, begin, size, rows),
        out_shape=[near_by(size, 2 * size), near_by(size, begin)],
        compiler_params=pltpu.CompilerParams(vmem_limit_bytes=vmem_bytes),
        name="open_block",
    )(kern, outer, before)


def close_kernel(begin, size, rows, done_ref, mixed_ref, before_ref, inv_ref, work):
    work[...] = done_ref[...]
    eliminate(work, size, rows, size)
    inverse = work[:, size:]
    before = before_ref[...]
    inv_ref[:begin, :begin] = before
    inv_ref[:begin, begin:] = jnp.zeros((begin, size), jnp.float32)
    inv_ref[begin:, begin:] = inverse
    inv_ref[begin:, :begin] = -contract(inverse, contract(mixed_ref[...], before, 1, 0, highest), 1, 0, highest)


def close_block(done, mixed, before, begin, size, rows):
    end = begin + size
    return pl.pallas_call(
        functools.partial(close_kernel, begin, size, rows),
        out_shape=near_by(end, end),
        scratch_shapes=[pltpu.VMEM((size, 2 * size), jnp.float32)],
        compiler_params=pltpu.CompilerParams(vmem_limit_bytes=vmem_bytes),
        name="close_block",
    )(done, mixed, before)


def columns_kernel(res_ref, inv_ref, *refs):
    out_ref, one, two, three = refs[-4:]

    @pl.when(pl.program_id(0) == 0)
    def _():
        one[...], two[...], three[...] = split3(inv_ref[...])

    a, b, c = split3(res_ref[...])
    out = contract(a, one[...], 1, 1) + (contract(a, two[...], 1, 1) + contract(b, one[...], 1, 1))
    out_ref[...] = out + (contract(b, two[...], 1, 1) + contract(a, three[...], 1, 1) + contract(c, one[...], 1, 1))


def new_columns(res, inv, made, tile, begin, end):
    count, total = res.shape
    in_specs = [
        pl.BlockSpec((tile, total), lambda i: (i + begin, 0)),
        pl.BlockSpec((total, total), lambda i: (0, 0)),
    ]
    args = (res, inv)
    if made is not None:
        in_specs.append(pl.BlockSpec(memory_space=pl.ANY))
        args = (res, inv, made)
    return pl.pallas_call(
        columns_kernel,
        grid=(end - begin,),
        in_specs=in_specs,
        out_specs=pl.BlockSpec((tile, total), lambda i: (i + begin, 0)),
        out_shape=jax.ShapeDtypeStruct((count, total), jnp.float32),
        scratch_shapes=[pltpu.VMEM((total, total), jnp.bfloat16)] * 3,
        input_output_aliases={} if made is None else {2: 0},
        compiler_params=pltpu.CompilerParams(vmem_limit_bytes=vmem_bytes),
        name="new_columns",
    )(*args)


def gram_kernel(count, mine_ref, other_ref, inv_ref, out_ref, sum_ref):
    join(sum_ref, mine_ref, other_ref)
    inv = inv_ref[...]
    rank = sum_ref.shape[1] - inv.shape[0]
    half = contract(inv, sum_ref[...], 1, 0, highest)
    out_ref[:, :rank] = half[:, :rank] / count
    out_ref[:, rank:] = contract(half[:, rank:], inv, 1, 1, highest) / count


def gram_rows(mine, other, inv, count):
    half, lanes = mine.shape
    return pl.pallas_call(
        functools.partial(gram_kernel, count),
        out_shape=jax.ShapeDtypeStruct((2 * half, lanes), jnp.float32),
        scratch_shapes=[pltpu.VMEM((2 * half, lanes), jnp.float32)],
        compiler_params=pltpu.CompilerParams(vmem_limit_bytes=vmem_bytes),
        name="gram_rows",
    )(mine, other, inv)


def sum_over_devices(keep, send, index, bits, work=None):
    def swap(pieces, masks):
        beside = work is not None and work.steps
        if beside:
            pieces, work.state = lax.optimization_barrier((pieces, work.state))
        got = [
            lax.ppermute(piece, AXES, [(i, i ^ mask) for i in range(1 << bits)]) for piece, mask in zip(pieces, masks)
        ]
        if beside:
            work.run()
            got, work.state = lax.optimization_barrier((got, work.state))
        return got

    four = [2, 4, 6]
    quarter = keep.shape[0] // 4
    place = (index >> 1) & 3
    x = keep + swap([send], [1])[0]
    parts = [lax.dynamic_slice_in_dim(x, (place ^ (mask >> 1)) * quarter, quarter, 0) for mask in four]
    x = lax.dynamic_slice_in_dim(x, place * quarter, quarter, 0)
    for got in swap(parts, four):
        x = x + got
    for bit in range(3, bits):
        x = x + swap([x], [1 << bit])[0]
    parts = [x] + swap([x] * 3, four)
    rows = []
    for spot in range(4):
        which = place ^ spot
        rows.append(jnp.where(which < 2, jnp.where(which == 0, parts[0], parts[1]), jnp.where(which == 2, parts[2], parts[3])))
    x = jnp.concatenate(rows, 0)
    return x, swap([x], [1])[0]


class Work:
    def __init__(self, state, steps):
        self.state = state
        self.steps = list(steps)

    def run(self):
        self.state = self.steps.pop(0)(self.state)


def body(bits, points, factor, pivots):
    count, width = points.shape
    blocks, size = pivots.shape
    index = position()
    points_t = pltpu.with_memory_space_constraint(points.T, pltpu.HBM)
    factor = pltpu.with_memory_space_constraint(factor, pltpu.HBM)
    fetched = sum_over_devices(*pick_rows(points_t, factor, pivots.reshape(-1)), index, bits)
    res, keep, send, pivot_rows = residuals(points_t, factor, *fetched)

    def pairs(state):
        return dict(state, pairs=pivot_pairs(state.pop("rows"), width))

    def first(state):
        return dict(state, inv=first_block(*state["pairs"], size))

    def open_next(begin):
        def run(state):
            return dict(state, open=open_block(*state["pairs"], state["inv"], begin, size, size // 2))

        return run

    def close_next(begin):
        def run(state):
            done, mixed = state.pop("open")
            return dict(state, inv=close_block(done, mixed, state["inv"], begin, size, size // 2))

        return run

    tile = min(1024, count)
    tiles = count // tile
    cuts = [0, tiles - tiles // 4, tiles]

    def columns(begin, end):
        def run(state):
            return dict(state, made=new_columns(state["res"], state["inv"], state["made"], tile, begin, end))

        return run

    steps = [pairs, first]
    for begin in range(size, blocks * size, size):
        steps += [open_next(begin), close_next(begin)]
    steps += [columns(b, e) for b, e in zip(cuts, cuts[1:]) if e > b]
    work = Work({"rows": pivot_rows, "res": res, "made": None}, steps)
    total = sum_over_devices(keep, send, index, bits, work)
    while work.steps:
        work.run()
    return work.state["made"], gram_rows(*total, work.state["inv"], count)


def solution(mesh):
    bits = (mesh.size - 1).bit_length()
    assert mesh.size == 1 << bits and bits >= 3
    in_specs = (P(AXES, None), P(AXES, None), P())
    out_specs = (P(AXES, None), P())
    return jax.shard_map(
        functools.partial(body, bits), mesh=mesh, in_specs=in_specs, out_specs=out_specs, check_vma=False
    )
```
